32 devices in a mesh: row: 8 (over y, x, core), col: 4 (over z).
Axes of the slice: x: 2, y: 2, z: 4, core: 2. Of those that a mesh axis runs over, the one named last changes fastest.
Arguments:
- species: bfloat16 [3, 512, 512, 256], P(None, 'row', 'col'), may hold values from -6 to 6
- flow_field: bfloat16 [3, 512, 512, 256], P(None, 'row', 'col'), may hold values from -6 to 6
- x_operators: bfloat16 [2, 512, 512], replicated, may hold values from -8 to 8
- y_operators: bfloat16 [2, 512, 512], replicated, may hold values from -8 to 8
Outputs:
- species_derivatives: bfloat16 [3, 2, 512, 512, 256], P(None, None, 'row', 'col')
- flow_derivatives: bfloat16 [3, 2, 512, 512, 256], P(None, None, 'row', 'col')
The draws below stay inside these ranges and needn't reach their ends.
All inputs are finite; a program needn't handle non-finite values.
Results may differ from the reference program's by a relative error of at most 0.001.
Values may be sent and summed in bfloat16 or wider, within the bound.
A program may use at most 256 MiB of HBM per device.

```python
import jax
import jax.numpy as jnp
from jax import lax

NX = 512
NY = 512
NZ = 256


def operator_pair(key, length):
    index = jnp.arange(length)
    offset = (index[None, :] - index[:, None]) % length

    def band(shift):
        return (offset == shift).astype(jnp.float32)
    ident = band(0)
    plus_one = band(1)
    minus_one = band(length - 1)
    plus_two = band(2)
    minus_two = band(length - 2)
    first_lhs = ident + (plus_one + minus_one) / 3.0
    first_rhs = 14.0 / 9.0 * (plus_one - minus_one) / 2.0 + 1.0 / 9.0 * (plus_two - minus_two) / 4.0
    second_lhs = ident + 2.0 / 11.0 * (plus_one + minus_one)
    second_rhs = 12.0 / 11.0 * (plus_one + minus_one - 2.0 * ident) + 3.0 / 11.0 * (plus_two + minus_two - 2.0 * ident) / 4.0
    first = jnp.linalg.solve(first_lhs, first_rhs)
    second = jnp.linalg.solve(second_lhs, second_rhs)
    keys = jax.random.split(key, 2)
    spacing = jnp.exp(jax.random.uniform(keys[0], (length,), jnp.float32, jnp.log(0.6), jnp.log(1.6)))
    extra = 0.5 * jax.random.normal(keys[1], (2, length, length), jnp.float32) / jnp.sqrt(length * 1.0)
    first = spacing[:, None] * first
    second = 0.25 * (spacing * spacing)[:, None] * second
    whole = jnp.stack([first, second]) + extra
    return jnp.clip(whole, -8.0, 8.0).astype(jnp.bfloat16)


def draw_x_operators(key, part):
    return operator_pair(jax.random.fold_in(key, 11), NX)


def draw_y_operators(key, part):
    return operator_pair(jax.random.fold_in(key, 23), NY)


def shard_levels(own_key, shape, shards, least, top_value):
    gain = 1.0
    for axis_at, shards_of in shards:
        draws = jax.random.uniform(jax.random.fold_in(jax.random.fold_in(own_key, 6), axis_at), (shards_of,), jnp.float32, least / len(shards), top_value / len(shards))
        gain = gain * jnp.repeat(jnp.exp(draws), shape[axis_at] // shards_of).reshape((-1,) + (1,) * (len(shape) - 1 - axis_at))
    return gain


def centred(own_key, dims, scale, limit, shards=(), dtype=jnp.bfloat16):
    array = scale * jax.random.normal(own_key, dims, jnp.float32)
    if shards:
        array = array * shard_levels(own_key, dims, shards, -0.22, 0.18)
    return jnp.clip(array, -limit, limit).astype(dtype)


def setup_inputs(seed: int = 0) -> dict:
    key_of = jax.random.split(jax.random.key(seed), 5)
    return {
        "species": centred(key_of[0], (3, NX, NY, NZ), 1.0, 6.0, ((1, 8), (2, 4))),
        "flow_field": centred(key_of[1], (3, NX, NY, NZ), 1.0, 6.0, ((1, 8), (2, 4))),
        "x_operators": draw_x_operators(jax.random.fold_in(key_of[4], 71), 0),
        "y_operators": draw_y_operators(jax.random.fold_in(key_of[4], 71), 0),
    }


def along_first(operators, field):
    ops = operators.astype(jnp.float32)
    values = field.astype(jnp.float32)
    first = jnp.einsum('ij,jyz->iyz', ops[0], values, precision=lax.Precision.HIGHEST)
    second = jnp.einsum('ij,jyz->iyz', ops[1], values, precision=lax.Precision.HIGHEST)
    return jnp.stack([first.astype(jnp.bfloat16), second.astype(jnp.bfloat16)])

def along_second(operators, field):
    ops = operators.astype(jnp.float32)
    values = field.astype(jnp.float32)
    first = jnp.einsum('ij,xjz->xiz', ops[0], values, precision=lax.Precision.HIGHEST)
    second = jnp.einsum('ij,xjz->xiz', ops[1], values, precision=lax.Precision.HIGHEST)
    return jnp.stack([first.astype(jnp.bfloat16), second.astype(jnp.bfloat16)])

def reference(species, flow_field, x_operators, y_operators):
    species_derivatives = lax.map(lambda field: along_first(x_operators, field), species)
    flow_derivatives = lax.map(lambda field: along_second(y_operators, field), flow_field)
    return (species_derivatives, flow_derivatives)
```

```python
import functools

import jax
import jax.numpy as jnp
from jax import lax
from jax.experimental import pallas as pl
from jax.experimental.pallas import tpu as pltpu
from jax.sharding import PartitionSpec as P


FLOW_SPLITS = 4
AHEAD = 3
BEHIND = 3
LAG = 1
VMEM = 56 * 1024 * 1024


def params():
    return pltpu.CompilerParams(vmem_limit_bytes=VMEM)


def cost(flops, moved):
    return pl.CostEstimate(flops=flops, bytes_accessed=moved, transcendentals=0)


TOKEN = jax.ShapeDtypeStruct((8, 128), jnp.float32)
TOKEN_SPEC = pl.BlockSpec((8, 128), lambda g: (0, 0))
ANY_SPEC = pl.BlockSpec(memory_space=pl.ANY)


def flow_kernel(count, ahead, w_ref, *refs):
    sources, (own_ref, served_ref) = refs[:count], refs[-2 - ahead :][:2]
    width = own_ref.shape[3]
    if ahead:
        refs[-1][...] = refs[count][0]

    @pl.loop(0, own_ref.shape[2])
    def _(x):
        lines = jnp.concatenate(
            [s[0, x] if len(s.shape) == 4 else s[x] for s in sources], axis=0
        )
        out = jnp.dot(w_ref[...], lines, preferred_element_type=jnp.float32)
        out = out.astype(jnp.bfloat16)
        for d in range(2):
            own_ref[0, d, x] = out[d * width : (d + 1) * width]
            served_ref[d, x] = out[(2 + d) * width : (3 + d) * width]


def flow_compute(weights, flow, received, s, start, rows, ahead, tokens):
    _, _, width, depth = flow.shape
    tile = min(rows, 4)
    block = pl.BlockSpec((tile, width, depth), lambda g: (g, 0, 0))

    def piece_of(s, start):
        return pl.BlockSpec((1, tile, width, depth), lambda g: (s, start // tile + g, 0, 0))

    n = weights.shape[1]
    later = [] if ahead is None else [ahead]
    return pl.pallas_call(
        functools.partial(flow_kernel, 1 + len(received), len(later)),
        grid=(rows // tile,),
        in_specs=[pl.BlockSpec(weights.shape, lambda g: (0, 0)), piece_of(s, start)]
        + [block] * len(received)
        + [piece_of(*at) for at in later]
        + [ANY_SPEC] * len(tokens),
        out_specs=[
            pl.BlockSpec((1, 2, tile, width, depth), lambda g: (0, 0, g, 0, 0)),
            pl.BlockSpec((2, tile, width, depth), lambda g: (0, g, 0, 0)),
        ]
        + [block] * len(later),
        out_shape=[
            jax.ShapeDtypeStruct((1, 2, rows, width, depth), jnp.bfloat16),
            jax.ShapeDtypeStruct((2, rows, width, depth), jnp.bfloat16),
        ]
        + [jax.ShapeDtypeStruct((rows, width, depth), jnp.bfloat16)] * len(later),
        compiler_params=params(),
        cost_estimate=cost(8 * rows * width * n * depth, 2 * rows * depth * (n + 4 * width)),
        name="flow_compute",
    )(weights, flow, *received, *[flow for _ in later], *tokens)


def pick_kernel(count, quarter, own_ref, got_ref, *refs):
    out_ref, token_ref = refs[-2:]
    me = lax.axis_index("col")
    inner = jnp.logical_and(me >= quarter, me < count - quarter)
    token_ref[...] = jnp.zeros_like(token_ref)

    @pl.when(inner)
    def _():
        out_ref[...] = own_ref[...]

    @pl.when(jnp.logical_not(inner))
    def _():
        out_ref[0] = got_ref[...]


def flow_pick(shape, own, got, whole, s, start, rows, count):
    tile = min(rows, 4)
    width, depth = shape[3:]
    operands = (own, got) + (() if whole is None else (whole,))
    return pl.pallas_call(
        functools.partial(pick_kernel, count, count // 4),
        grid=(rows // tile,),
        in_specs=[
            pl.BlockSpec((1, 2, tile, width, depth), lambda g: (0, 0, g, 0, 0)),
            pl.BlockSpec((2, tile, width, depth), lambda g: (0, g, 0, 0)),
        ]
        + [ANY_SPEC] * (len(operands) - 2),
        out_specs=[
            pl.BlockSpec(
                (1, 2, tile, width, depth), lambda g: (s, 0, start // tile + g, 0, 0)
            ),
            TOKEN_SPEC,
        ],
        out_shape=[jax.ShapeDtypeStruct(shape, jnp.bfloat16), TOKEN],
        input_output_aliases={2: 0} if whole is not None else {},
        compiler_params=params(),
        cost_estimate=cost(0, 12 * rows * width * depth),
        name="flow_pick",
    )(*operands)


def turn_kernel(in_ref, out_ref, scratch):
    _, width, tile, depth = in_ref.shape
    for h in range(depth // 128):
        part = in_ref[0, :, :, h * 128 : (h + 1) * 128].astype(jnp.float32)
        scratch[h] = part.reshape(width * tile, 128)
    for y in range(tile):
        for h in range(depth // 128):
            out_ref[y, :, h * 128 : (h + 1) * 128] = scratch[
                h, pl.ds(y, width, stride=tile), :
            ].astype(jnp.bfloat16)


def turn(species, s):
    _, width, rows, depth = species.shape
    tile = 16
    return pl.pallas_call(
        turn_kernel,
        grid=(rows // tile,),
        in_specs=[pl.BlockSpec((1, width, tile, depth), lambda g: (s, 0, g, 0))],
        out_specs=pl.BlockSpec((tile, width, depth), lambda g: (g, 0, 0)),
        out_shape=jax.ShapeDtypeStruct((rows, width, depth), jnp.bfloat16),
        scratch_shapes=[pltpu.VMEM((depth // 128, width * tile, 128), jnp.float32)],
        compiler_params=params(),
        cost_estimate=cost(0, 4 * rows * width * depth),
        name="turn",
    )(species)


def species_kernel(w_ref, lines_ref, *refs):
    out_ref, token_ref, scratch = refs[-3:]
    _, _, width, tile, depth = out_ref.shape
    token_ref[...] = jnp.zeros_like(token_ref)

    for y in range(tile):
        lines = jnp.concatenate([lines_ref[k, y] for k in range(lines_ref.shape[0])], axis=0)
        out = jnp.dot(w_ref[...], lines, preferred_element_type=jnp.float32)
        for h in range(depth // 128):
            scratch[h, pl.ds(y, 2 * width, stride=tile), :] = out[:, h * 128 : (h + 1) * 128]
    for h in range(depth // 128):
        for d in range(2):
            part = scratch[h, d * width * tile : (d + 1) * width * tile, :]
            out_ref[0, d, :, :, h * 128 : (h + 1) * 128] = part.reshape(
                width, tile, 128
            ).astype(jnp.bfloat16)


def species_compute(shape, weights, lines, whole, s, start, tokens):
    _, _, width, _, depth = shape
    count, rows = lines.shape[:2]
    tile = 16
    operands = (weights, lines) + (() if whole is None else (whole,)) + tuple(tokens)
    n = weights.shape[1]
    return pl.pallas_call(
        species_kernel,
        grid=(rows // tile,),
        in_specs=[
            pl.BlockSpec(weights.shape, lambda g: (0, 0)),
            pl.BlockSpec((count, tile, width, depth), lambda g: (0, g, 0, 0)),
        ]
        + [ANY_SPEC] * (len(operands) - 2),
        out_specs=[
            pl.BlockSpec(
                (1, 2, width, tile, depth), lambda g: (s, 0, 0, start // tile + g, 0)
            ),
            TOKEN_SPEC,
        ],
        out_shape=[jax.ShapeDtypeStruct(shape, jnp.bfloat16), TOKEN],
        scratch_shapes=[pltpu.VMEM((depth // 128, 2 * width * tile, 128), jnp.float32)],
        input_output_aliases={2: 0} if whole is not None else {},
        compiler_params=params(),
        cost_estimate=cost(4 * rows * width * n * depth, 2 * rows * depth * (n + 2 * width)),
        name="species_compute",
    )(*operands)


def operator_rows(operators, count, row, columns):
    width = operators.shape[1] // count
    rows = lax.dynamic_slice_in_dim(operators, row * width, width, axis=1)
    parts = [lax.dynamic_slice_in_dim(rows, c * width, width, axis=2) for c in columns]
    return jnp.concatenate(parts, axis=2).reshape(2 * width, count * width)


def body(rows_n, cols_n, species, flow, x_operators, y_operators):
    kinds, width_x, width_y, depth = species.shape
    out_shape = (kinds, 2, width_x, width_y, depth)

    quarter, half = cols_n // 4, cols_n // 2
    inner = [quarter + i for i in range(half)]
    outer = [i if i < quarter else i + half for i in range(half)]
    at = jnp.clip(lax.axis_index("col") - quarter, 0, half - 1)

    def inner_of(i):
        return quarter + i

    def outer_of(i):
        return jnp.where(i < quarter, i, i + half)

    plans, columns = [], [inner_of(at)]
    for k in range(half):
        plans.append([(outer[i], inner[(i + k) % half]) for i in range(half)])
        columns.append(outer_of((at - k) % half))
    for k in range(1, half):
        plans.append([(inner[i], inner[(i + k) % half]) for i in range(half)])
        columns.append(inner_of((at - k) % half))
    back = [(inner[i], outer[i]) for i in range(half)]
    y_weights = jnp.concatenate(
        [operator_rows(y_operators, cols_n, o, columns) for o in (inner_of(at), outer_of(at))]
    )

    row = lax.axis_index("row")
    x_weights = lax.dynamic_slice_in_dim(x_operators, row * width_x, width_x, axis=1)
    x_weights = x_weights.reshape(2 * width_x, rows_n * width_x)
    lines = [lax.all_gather(turn(species, s), "row") for s in range(kinds)]

    flow_rows = width_x // FLOW_SPLITS
    chunks = [(s, c * flow_rows) for s in range(kinds) for c in range(FLOW_SPLITS)]
    pieces = [flow[s, start : start + flow_rows] for s, start in chunks[:AHEAD]]
    received = [[lax.ppermute(piece, "col", plan) for plan in plans] for piece in pieces]

    when = {((s + 1) * len(chunks)) // kinds + LAG: s for s in range(kinds)}
    species_out, flow_out, results, order = None, None, [], []

    def multiply(s, after):
        return species_compute(out_shape, x_weights, lines[s], species_out, s, 0, after)

    def pick(k):
        s, start = chunks[k]
        return flow_pick(out_shape, *results[k], flow_out, s, start, flow_rows, cols_n)

    for k, (s, start) in enumerate(chunks):
        tokens = order
        if k in when:
            species_out, token = multiply(when[k], tokens)
            tokens = [token]
        ahead = chunks[k + AHEAD] if k + AHEAD < len(chunks) else None
        own, served, *piece = flow_compute(
            y_weights, flow, received[k], s, start, flow_rows, ahead, tokens
        )
        received.extend([lax.ppermute(p, "col", plan) for plan in plans] for p in piece)
        results.append((own, lax.ppermute(served, "col", back)))
        order = []
        if k >= BEHIND:
            flow_out, token = pick(k - BEHIND)
            order = [token]
    for k, s in when.items():
        if k >= len(chunks):
            species_out, token = multiply(s, order)
            order = [token]
    for k in range(len(chunks) - BEHIND, len(chunks)):
        flow_out, _ = pick(k)
    return (species_out, flow_out)


def solution(mesh):
    placed = (P(None, "row", "col", None), P(None, "row", "col", None), P(), P())
    return jax.shard_map(
        functools.partial(body, mesh.shape["row"], mesh.shape["col"]),
        mesh=mesh,
        in_specs=placed,
        out_specs=(P(None, None, "row", "col", None), P(None, None, "row", "col", None)),
        check_vma=False,
    )
```
